128 devices in a mesh: day: 16 (over x, y), pair: 8 (over z, core).
Axes of the slice: x: 4, y: 4, z: 4, core: 2. Of those that a mesh axis runs over, the one named last changes fastest.
Arguments:
- correlations: bfloat16 [64, 4096, 2001], P('day', 'pair'), may hold values from -8 to 8
- mask: int32 [64, 4096], P('day', 'pair'), may hold values from 0 to 1, as said below
- counts: int32 [4096], P(('pair', 'day')), may hold values from 1 to 64, as said below
Outputs:
- phase_weighted: float32 [4096, 2001], P(('pair', 'day'))
- linear: float32 [4096, 2001], P(('pair', 'day'))
The draws below stay inside these ranges and needn't reach their ends.
Inputs may be any that keep to these rules, and one draw needn't show every extreme that they name: `mask`: every pair has a usable correlation on at least one day. counts[p] equals the number of days d with mask[d, p] = 1.
All inputs are finite; a program needn't handle non-finite values.
Results may differ from the reference program's by a relative error of at most 0.00044.
Values may be sent and summed in bfloat16 or wider, within the bound.
A program may use at most 128 MiB of HBM per device.

```python
import jax
import jax.numpy as jnp
from jax import lax

LAGS = 2001
DAYS = 64
PAIRS = 4096


def mask_pair(key):
    base = jax.random.fold_in(key, 7)
    keys = jax.random.split(base, 5)
    day_rate = jax.random.randint(keys[0], (DAYS,), 30, 101)
    pair_rate = jax.random.randint(keys[1], (PAIRS,), 40, 101)
    draws = jax.random.randint(keys[2], (DAYS, PAIRS), 0, 10000)
    usable = (draws < day_rate[:, None] * pair_rate[None, :]).astype(jnp.int32)
    forced = jax.random.randint(keys[3], (PAIRS,), 0, DAYS)
    chosen = (jnp.arange(DAYS)[:, None] == forced[None, :]).astype(jnp.int32)
    usable = jnp.maximum(usable, chosen)
    full_pair = jax.random.randint(keys[4], (), 0, PAIRS)
    always = (jnp.arange(PAIRS) == full_pair).astype(jnp.int32)
    usable = jnp.maximum(usable, always[None, :])
    return (usable, jnp.sum(usable, axis=0).astype(jnp.int32))


def draw_mask(key, part):
    return mask_pair(key)[0]


def draw_counts(key, part):
    return mask_pair(key)[1]


def draw_correlations(key, part):
    keys = jax.random.split(jax.random.fold_in(key, 3), 5)
    block_index = jnp.arange(PAIRS) // 64
    block_total = (PAIRS + 63) // 64
    pair_scale = jnp.exp(jax.random.uniform(keys[0], (PAIRS,), jnp.float32, -0.8, 0.8))
    block_scale = jnp.exp(jax.random.uniform(keys[1], (block_total,), jnp.float32, -0.8, 0.8))[block_index]
    day_scale = jnp.exp(jax.random.uniform(keys[2], (DAYS,), jnp.float32, -0.7, 0.7))
    signal = 0.7 * jax.random.normal(keys[3], (PAIRS, LAGS), jnp.float32)
    noise = jax.random.normal(keys[4], (DAYS, PAIRS, LAGS), jnp.float32)
    values = day_scale[:, None, None] * (pair_scale * block_scale)[None, :, None] * (signal[None] + noise)
    return jnp.clip(values, -8.0, 8.0).astype(jnp.bfloat16)


def setup_inputs(seed: int = 0) -> dict:
    seeds = jax.random.split(jax.random.key(seed), 4)
    correlations = draw_correlations(jax.random.fold_in(seeds[3], 71), 0)
    mask = draw_mask(jax.random.fold_in(seeds[3], 71), 0)
    counts = draw_counts(jax.random.fold_in(seeds[3], 71), 0)
    return dict(correlations=correlations, mask=mask, counts=counts)


def hilbert_kernel():
    offset = jnp.arange(LAGS, dtype=jnp.int32)
    offset = jnp.where(offset > LAGS // 2, offset - LAGS, offset)
    phase_angle = jnp.pi * offset.astype(jnp.float32) / LAGS
    parity = 1.0 - 2.0 * (offset % 2).astype(jnp.float32)
    sine_safe = jnp.where(offset == 0, 1.0, jnp.sin(phase_angle))
    kernel = jnp.where(offset == 0, 0.0, (jnp.cos(phase_angle) - parity) / (LAGS * sine_safe))
    rounded = lax.optimization_barrier(kernel.astype(jnp.bfloat16))
    return rounded.astype(jnp.float32)

def hilbert_part(day_rows, kernel_spectrum):
    spectrum = jnp.fft.fft(day_rows, axis=-1)
    return jnp.real(jnp.fft.ifft(spectrum * kernel_spectrum, axis=-1))

def reference(correlations, mask, counts):
    masked = correlations * mask[:, :, None].astype(jnp.bfloat16)
    energy = lax.map(lambda day_rows: jnp.sum(jnp.square(day_rows.astype(jnp.float32))), masked)
    used_pairs = lax.optimization_barrier(jnp.sum(mask, axis=1)).astype(jnp.float32)
    weight = 1.0 / jnp.sqrt(energy / (LAGS * jnp.maximum(used_pairs, 1.0)) + 0.1)
    kernel_spectrum = jnp.fft.fft(hilbert_kernel())

    def add_day(totals, inputs):
        day_rows, day_weight = inputs
        values = day_rows.astype(jnp.float32)
        real_part = day_weight * values
        imag_part = day_weight * hilbert_part(values, kernel_spectrum)
        amplitude = jnp.sqrt(real_part * real_part + imag_part * imag_part + 0.25)
        return ((totals[0] + real_part, totals[1] + real_part / amplitude, totals[2] + imag_part / amplitude), None)
    zeros = jnp.zeros((PAIRS, LAGS), jnp.float32)
    totals, unused = lax.scan(add_day, (zeros, zeros, zeros), (masked, weight))
    divisor = jnp.maximum(counts.astype(jnp.float32), 1.0)[:, None]
    linear = totals[0] / divisor
    coherence = (totals[1] * totals[1] + totals[2] * totals[2]) / (divisor * divisor)
    return (linear * coherence, linear)
```

```python
import jax
import jax.numpy as jnp
from jax import lax
from jax.experimental import pallas as pl
from jax.experimental.pallas import tpu as pltpu
from jax.sharding import PartitionSpec as P

BF = jnp.bfloat16
F32 = jnp.float32
MESH = pl.DeviceIdType.MESH
LAGS = 2001
WIDE = 2048


def alpha(v):
    return v + 1 - 2 * (v % 2)


def beta(v):
    return 3 - v


def hilbert_rows():
    u = lax.broadcasted_iota(jnp.int32, (8, 4096), 1)
    s = lax.broadcasted_iota(jnp.int32, (8, 4096), 0)
    t = jnp.where(u < 3840, u, u - 4096) - 1792 - s
    offset = (t + 4 * LAGS) % LAGS
    offset = jnp.where(offset > LAGS // 2, offset - LAGS, offset)
    phase_angle = jnp.pi * offset.astype(F32) / LAGS
    parity = 1.0 - 2.0 * (offset % 2).astype(F32)
    sine_safe = jnp.where(offset == 0, 1.0, jnp.sin(phase_angle))
    return jnp.where(offset == 0, 0.0, (jnp.cos(phase_angle) - parity) / (LAGS * sine_safe))


def kernel(x_hbm, mask_ref, counts_ref, rows_ref, pw_ref, lin_ref,
           slab, flat, xr, r1, table, s1, s2, r2, r3, r4, en, ww, wn,
           in_sem, a_s, a_r, b_s, b_r, c_s, c_r, d_s, d_r, e_s, e_r, w_s, w_r):
    day = lax.axis_index("day")
    pair = lax.axis_index("pair")
    x = day // 4
    y = day % 4
    xa, xb, ya, yb = alpha(x), beta(x), alpha(y), beta(y)
    x2, y2 = (x + 2) % 4, (y + 2) % 4
    along_x_a, along_x_b = (x, xa, xb, x2), (x, xb, xa, x2)
    along_y_a, along_y_b = (y, ya, yb, y2), (y, yb, ya, y2)
    firsts = (along_x_a, along_x_b, along_y_a, along_y_b)
    seconds = (along_y_a, along_y_b, along_x_a, along_x_b)

    def at_first(c, v):
        return (v * 4 + y, pair) if c < 2 else (x * 4 + v, pair)

    def at_second(c, v):
        return (x * 4 + v, pair) if c < 2 else (v * 4 + y, pair)

    neighbours = [(xa * 4 + y, pair), (xb * 4 + y, pair), (x * 4 + ya, pair), (x * 4 + yb, pair)]
    peers = [(day, (pair + k) % 8) for k in range(1, 8)]

    def load_block(i, cb):
        cols = pl.ds(pl.multiple_of(cb * 128, 128), 128)
        return pltpu.make_async_copy(x_hbm.at[:, :, cols], slab.at[i], in_sem.at[i])

    order = (x2, xa, xb, x)
    loads = [load_block(i, cb) for i, cb in enumerate(order)]
    for load in loads:
        load.start()

    barrier = pltpu.get_barrier_semaphore()
    for to in neighbours + peers:
        pl.semaphore_signal(barrier, inc=1, device_id=to, device_id_type=MESH)

    flat[pl.ds(8000, 192), :] = jnp.zeros((192, 128), F32)

    def remote(src, dst, send, recv, to):
        return pltpu.make_async_remote_copy(
            src_ref=src, dst_ref=dst, send_sem=send, recv_sem=recv, device_id=to, device_id_type=MESH
        )

    def raw_block(c, g, a):
        return remote(xr.at[c, a], r1.at[c, g], a_s.at[c, g], a_r.at[c, g], at_first(c, firsts[c][1]))

    def raw_piece(c, g, a, b):
        return remote(xr.at[c, a, b], r1.at[c, g, b], a_s.at[c, g], a_r.at[c, g], at_first(c, firsts[c][1]))

    squares = jnp.zeros((8, 128), F32)
    used = jnp.zeros((8, 128), F32)
    for i, cb in enumerate(order):
        loads[i].wait()
        cols = pl.ds(pl.multiple_of(cb * 128, 128), 128)
        m4 = mask_ref[:, cols].astype(F32)
        m8 = jnp.concatenate([m4, m4], axis=0)
        used = used + m8
        rows = slab.at[i].reshape(4 * LAGS, 128)

        def widen(j, acc, rows=rows, m8=m8):
            at = pl.ds(pl.multiple_of(j * 32, 32), 32)
            v = rows[at, :].astype(F32).reshape(4, 8, 128) * m8[None]
            flat[at, :] = v.reshape(32, 128)
            return acc + jnp.sum(v * v, axis=0)

        squares = lax.fori_loop(0, 250, widen, squares, unroll=10)
        last = rows[pl.ds(8000, 4), :].astype(F32) * m4
        flat[pl.ds(8000, 4), :] = last
        squares = squares + jnp.concatenate([last * last, jnp.zeros((4, 128), F32)], axis=0)

        def turn(j, carry, cb=cb):
            lags = pl.ds(pl.multiple_of(j * 128, 128), 128)
            for d in range(4):
                t = flat[pl.ds(pl.multiple_of(j * 512, 512) + d, 128, stride=4), :]
                t = t.astype(BF).T.reshape(4, 4, 8, 128)
                for c in range(2):
                    xr[c, cb, :, d, :, lags] = t[:, c]
                for c in range(2, 4):
                    for q in range(4):
                        xr[c, q, cb, d, :, lags] = t[q, c]
            return carry

        lax.fori_loop(0, 16, turn, 0, unroll=2)
        if i == 0:
            pl.semaphore_wait(barrier, len(neighbours) + len(peers))
            for c in range(2):
                raw_block(c, 0, x2).start()
        if i == 1:
            raw_block(0, 1, xa).start()
        if i == 2:
            raw_block(1, 1, xb).start()
        for c in range(2, 4):
            raw_piece(c, 0, y2, cb).start()
    for c in range(2, 4):
        for cb in order:
            raw_piece(c, 1, firsts[c][1], cb).start()

    en[0, 0] = squares
    en[0, 1] = used
    energy_copies = [
        remote(en.at[0], en.at[k], e_s.at[k], e_r.at[k], peers[k - 1]) for k in range(1, 8)
    ]
    for copy in energy_copies:
        copy.start()

    def tabulate(j, carry):
        lo = pltpu.roll(rows_ref[...], j * 16, 1)
        hi = pltpu.roll(rows_ref[...], j * 16 + 8, 1)
        both = jnp.concatenate([lo, hi], axis=0).astype(BF)
        for a in range(8):
            table[pl.ds(pl.multiple_of(a * 256 + j * 16, 16), 16), :] = both[:, 256 * (7 - a) : 256 * (7 - a) + WIDE]
        return carry

    lax.fori_loop(0, 16, tabulate, 0)

    for copy in energy_copies:
        copy.wait_recv()
    total = jnp.sum(en[:, 0], axis=0)
    pairs_used = jnp.sum(en[:, 1], axis=0)
    energy = jnp.sum(total[:4] + total[4:], axis=1, keepdims=True)
    pairs_used = jnp.sum(pairs_used[:4], axis=1, keepdims=True)
    level = energy / (LAGS * jnp.maximum(pairs_used, 1.0)) + 0.1
    weight = lax.rsqrt(level)
    for d in range(4):
        ww[0, d] = jnp.broadcast_to(weight[d : d + 1], (8, 128))
        ww[1, d] = jnp.broadcast_to(0.25 * level[d : d + 1], (8, 128))
    weight_copies = [remote(ww, wn.at[k], w_s.at[k], w_r.at[k], neighbours[k]) for k in range(4)]
    for copy in weight_copies:
        copy.start()
    for copy in weight_copies:
        copy.wait_recv()

    def stack(c, g, out):
        a = firsts[c][2] if g == 0 else firsts[c][0]
        raw_block(c, g, a).wait_recv()

        def tile(n, carry):
            cols = pl.ds(pl.multiple_of(n * 256, 256), 256)
            lhs = jnp.concatenate(
                [xr[c, a].reshape(128, WIDE), r1[c, g].reshape(128, WIDE)], axis=0
            )
            h = jnp.dot(lhs, table[:, cols], preferred_element_type=F32)
            for b in range(4):
                sums = [jnp.zeros((8, 256), F32)] * 3
                for s in range(2):
                    for d in range(4):
                        at = s * 128 + b * 32 + d * 8
                        hh = h[at : at + 8]
                        xx = (xr[c, a, b, d, :, cols] if s == 0 else r1[c, g, b, d, :, cols]).astype(F32)
                        w = ww[0, d] if s == 0 else wn[c, 0, d]
                        q = ww[1, d] if s == 0 else wn[c, 1, d]
                        w = jnp.concatenate([w, w], axis=1)
                        q = jnp.concatenate([q, q], axis=1)
                        inverse = lax.rsqrt(xx * xx + hh * hh + q)
                        sums = [sums[0] + w * xx, sums[1] + xx * inverse, sums[2] + hh * inverse]
                for k in range(3):
                    out[c, b, k, :, cols] = sums[k]
            return carry

        lax.fori_loop(0, 8, tile, 0)

    def second_order(c):
        v, q1, q2, v2 = seconds[c]
        return (v2, q1, q2, v)

    def sums_first(c, k):
        b = second_order(c)[k]
        return remote(s1.at[c, b], r2.at[c, b], b_s.at[c, k], b_r.at[c, k], at_first(c, firsts[c][2]))

    def sums_second(c, k):
        b = second_order(c)[k]
        return remote(s2.at[c, b], r3.at[c, k], c_s.at[c, k], c_r.at[c, k], at_second(c, seconds[c][1]))

    def sums_third(c):
        b = second_order(c)[2]
        return remote(s2.at[c, b], r4.at[c], d_s.at[c], d_r.at[c], at_second(c, seconds[c][2]))

    def stage_three(c):
        for k in range(2):
            b = second_order(c)[k]
            sums_first(c, k).wait_recv()
            s2[c, b] = s2[c, b] + r2[c, b]
            sums_second(c, k).start()

    def stage_four(c):
        b = second_order(c)[2]
        sums_first(c, 2).wait_recv()
        sums_second(c, 0).wait_recv()
        s2[c, b] = s2[c, b] + r2[c, b] + r3[c, 0]
        sums_third(c).start()

    def finish(c):
        b = second_order(c)[3]
        sums_first(c, 3).wait_recv()
        sums_second(c, 1).wait_recv()
        sums_third(c).wait_recv()
        linear, real, imag = [s2[c, b, k] + r2[c, b, k] + r3[c, 1, k] + r4[c, k] for k in range(3)]
        n = counts_ref[pl.ds(8 * c, 8), :]
        n = jnp.concatenate([n] * 16, axis=1)
        linear = linear / n
        lin_ref[pl.ds(8 * c, 8), :] = linear[:, :LAGS]
        pw_ref[pl.ds(8 * c, 8), :] = (linear * ((real * real + imag * imag) / (n * n)))[:, :LAGS]

    for c in range(4):
        stack(c, 0, s1)
        for k in range(4):
            sums_first(c, k).start()
    for c in range(4):
        stack(c, 1, s2)
        if c:
            stage_three(c - 1)
    stage_three(3)
    for c in range(4):
        stage_four(c)
    for c in range(4):
        finish(c)

    for copy in energy_copies + weight_copies:
        copy.wait_send()
    for c in range(4):
        for g in range(2):
            raw_block(c, g, x).wait_send()
        for k in range(4):
            sums_first(c, k).wait_send()
        for k in range(2):
            sums_second(c, k).wait_send()
        sums_third(c).wait_send()


def shards(correlations, mask, counts):
    lag_major = jnp.transpose(correlations, (2, 0, 1))
    divisor = jnp.broadcast_to(jnp.maximum(counts.astype(F32), 1.0)[:, None], (32, 128))
    vmem = pl.BlockSpec(memory_space=pltpu.VMEM)
    dma = pltpu.SemaphoreType.DMA
    return pl.pallas_call(
        kernel,
        out_shape=[jax.ShapeDtypeStruct((32, LAGS), F32)] * 2,
        in_specs=[pl.BlockSpec(memory_space=pl.ANY), vmem, vmem, vmem],
        out_specs=[vmem, vmem],
        scratch_shapes=[
            pltpu.VMEM((4, LAGS, 4, 128), BF),
            pltpu.VMEM((8192, 128), F32),
            pltpu.VMEM((4, 4, 4, 4, 8, WIDE), BF),
            pltpu.VMEM((4, 2, 4, 4, 8, WIDE), BF),
            pltpu.VMEM((WIDE, WIDE), BF),
            pltpu.VMEM((4, 4, 3, 8, WIDE), F32),
            pltpu.VMEM((4, 4, 3, 8, WIDE), F32),
            pltpu.VMEM((4, 4, 3, 8, WIDE), F32),
            pltpu.VMEM((4, 2, 3, 8, WIDE), F32),
            pltpu.VMEM((4, 3, 8, WIDE), F32),
            pltpu.VMEM((8, 2, 8, 128), F32),
            pltpu.VMEM((2, 4, 8, 128), F32),
            pltpu.VMEM((4, 2, 4, 8, 128), F32),
            dma((4,)),
            dma((4, 2)), dma((4, 2)),
            dma((4, 4)), dma((4, 4)),
            dma((4, 2)), dma((4, 2)),
            dma((4,)), dma((4,)),
            dma((8,)), dma((8,)),
            dma((4,)), dma((4,)),
        ],
        compiler_params=pltpu.CompilerParams(
            collective_id=0, has_side_effects=True, vmem_limit_bytes=67043328
        ),
    )(lag_major, mask, divisor, hilbert_rows())


def solution(mesh):
    placed = (P("day", "pair", None), P("day", "pair"), P(("pair", "day")))
    return jax.shard_map(
        shards,
        mesh=mesh,
        in_specs=placed,
        out_specs=(P(("pair", "day"), None), P(("pair", "day"), None)),
        check_vma=False,
    )
```

```python
import jax
import jax.numpy as jnp
from jax import lax
from jax.experimental import pallas as pl
from jax.experimental.pallas import tpu as pltpu
from jax.sharding import PartitionSpec as P

BF = jnp.bfloat16
F32 = jnp.float32
MESH = pl.DeviceIdType.MESH
LAGS = 2001
WIDE = 2048


def alpha(v):
    return v + 1 - 2 * (v % 2)


def beta(v):
    return 3 - v


def hilbert_rows():
    u = lax.broadcasted_iota(jnp.int32, (8, 4096), 1)
    s = lax.broadcasted_iota(jnp.int32, (8, 4096), 0)
    t = jnp.where(u < 3840, u, u - 4096) - 1792 - s
    offset = jnp.where(t > LAGS // 2, t - LAGS, jnp.where(t < -(LAGS // 2), t + LAGS, t))
    phase_angle = jnp.pi * offset.astype(F32) / LAGS
    parity = 1.0 - 2.0 * (offset & 1).astype(F32)
    sine_safe = jnp.where(offset == 0, 1.0, jnp.sin(phase_angle))
    return jnp.where(offset == 0, 0.0, (jnp.cos(phase_angle) - parity) / (LAGS * sine_safe))


def kernel(x_hbm, mask_ref, sums_ref,
           slab, flat, xr, r1, table, s1, s2, coded, r2, r3, r4, en, ww, wn, unit, hil, rows_ref,
           in_sem, a_s, a_r, b_s, b_r, c_s, c_r, d_s, d_r, e_s, e_r, w_s, w_r):
    day = lax.axis_index("day")
    pair = lax.axis_index("pair")
    x = day // 4
    y = day % 4
    xa, xb, ya, yb = alpha(x), beta(x), alpha(y), beta(y)
    x2, y2 = (x + 2) % 4, (y + 2) % 4
    along_x_a, along_x_b = (x, xa, xb, x2), (x, xb, xa, x2)
    along_y_a, along_y_b = (y, ya, yb, y2), (y, yb, ya, y2)
    firsts = (along_x_a, along_x_b, along_y_a, along_y_b)
    seconds = (along_y_a, along_y_b, along_x_a, along_x_b)

    def at_first(c, v):
        return (v * 4 + y, pair) if c < 2 else (x * 4 + v, pair)

    def at_second(c, v):
        return (x * 4 + v, pair) if c < 2 else (v * 4 + y, pair)

    neighbours = [(xa * 4 + y, pair), (xb * 4 + y, pair), (x * 4 + ya, pair), (x * 4 + yb, pair)]
    peers = [(day, (pair + k) % 8) for k in range(1, 8)]

    def load_block(i, cb):
        cols = pl.ds(pl.multiple_of(cb * 128, 128), 128)
        return pltpu.make_async_copy(x_hbm.at[:, :, cols], slab.at[i], in_sem.at[i])

    order = (x2, xa, xb, x)
    loads = [load_block(i, cb) for i, cb in enumerate(order)]
    loads[0].start()

    barrier = pltpu.get_barrier_semaphore()
    for to in neighbours + peers:
        pl.semaphore_signal(barrier, inc=1, device_id=to, device_id_type=MESH)

    flat[pl.ds(8000, 192), :] = jnp.zeros((192, 128), F32)
    rows_ref[...] = hilbert_rows()

    def remote(src, dst, send, recv, to):
        return pltpu.make_async_remote_copy(
            src_ref=src, dst_ref=dst, send_sem=send, recv_sem=recv, device_id=to, device_id_type=MESH
        )

    def raw_block(c, g, a):
        return remote(xr.at[c, a], r1.at[c, g], a_s.at[c, g], a_r.at[c, g], at_first(c, firsts[c][1]))

    def raw_piece(c, g, a, b):
        return remote(xr.at[c, a, b], r1.at[c, g, b], a_s.at[c, g], a_r.at[c, g], at_first(c, firsts[c][1]))

    squares = jnp.zeros((8, 128), F32)
    used = jnp.zeros((8, 128), F32)
    for i, cb in enumerate(order):
        loads[i].wait()
        if i < 3:
            loads[i + 1].start()
        cols = pl.ds(pl.multiple_of(cb * 128, 128), 128)
        m4 = mask_ref[:, cols].astype(F32)
        m8 = jnp.concatenate([m4, m4], axis=0)
        used = used + m8
        rows = slab.at[i].reshape(4 * LAGS, 128)

        def widen(j, acc, rows=rows, m8=m8):
            at = pl.ds(pl.multiple_of(j * 32, 32), 32)
            v = rows[at, :].astype(F32).reshape(4, 8, 128) * m8[None]
            flat[at, :] = v.reshape(32, 128)
            return acc + jnp.sum(v * v, axis=0)

        squares = lax.fori_loop(0, 250, widen, squares, unroll=10)
        last = rows[pl.ds(8000, 4), :].astype(F32) * m4
        flat[pl.ds(8000, 4), :] = last
        squares = squares + jnp.concatenate([last * last, jnp.zeros((4, 128), F32)], axis=0)

        def turn(j, carry, cb=cb):
            lags = pl.ds(pl.multiple_of(j * 128, 128), 128)
            for d in range(4):
                t = flat[pl.ds(pl.multiple_of(j * 512, 512) + d, 128, stride=4), :]
                t = t.astype(BF).T.reshape(4, 4, 8, 128)
                for c in range(2):
                    xr[c, cb, :, d, :, lags] = t[:, c]
                for c in range(2, 4):
                    for q in range(4):
                        xr[c, q, cb, d, :, lags] = t[q, c]
            return carry

        lax.fori_loop(0, 16, turn, 0, unroll=2)
        if i == 0:
            pl.semaphore_wait(barrier, len(neighbours) + len(peers))
            for c in range(2):
                raw_block(c, 0, x2).start()
        for c in range(2, 4):
            raw_piece(c, 0, y2, cb).start()

    en[0, 0] = squares
    en[0, 1] = used
    energy_copies = [
        remote(en.at[0], en.at[k], e_s.at[k], e_r.at[k], peers[k - 1]) for k in range(1, 8)
    ]
    for copy in energy_copies:
        copy.start()

    def tabulate(j, carry):
        lo = pltpu.roll(rows_ref[...], j * 16, 1)
        hi = pltpu.roll(rows_ref[...], j * 16 + 8, 1)
        both = jnp.concatenate([lo, hi], axis=0).astype(BF)
        for a in range(8):
            table[pl.ds(pl.multiple_of(a * 256 + j * 16, 16), 16), :] = both[:, 256 * (7 - a) : 256 * (7 - a) + WIDE]
        return carry

    lax.fori_loop(0, 16, tabulate, 0)

    for copy in energy_copies:
        copy.wait_recv()
    total = jnp.sum(en[:, 0], axis=0)
    pairs_used = jnp.sum(en[:, 1], axis=0)
    energy = jnp.sum(total[:4] + total[4:], axis=1, keepdims=True)
    pairs_used = jnp.sum(pairs_used[:4], axis=1, keepdims=True)
    level = energy / (LAGS * jnp.maximum(pairs_used, 1.0)) + 0.1
    weight = lax.rsqrt(level)
    reach = weight * jnp.sqrt(energy)
    for d in range(4):
        ww[0, d] = jnp.broadcast_to(weight[d : d + 1], (8, 128))
        ww[1, d] = jnp.broadcast_to(0.25 * level[d : d + 1], (8, 128))
        ww[2, d] = jnp.broadcast_to(reach[d : d + 1], (8, 128))
    weight_copies = [remote(ww, wn.at[k], w_s.at[k], w_r.at[k], neighbours[k]) for k in range(4)]
    for copy in weight_copies:
        copy.start()
    for c in range(4):
        raw_block(c, 1, firsts[c][1]).start()

    def scale_up(c):
        reach = jnp.maximum(jnp.max(ww[2], axis=0), jnp.max(wn[c, 2], axis=0))
        units = jnp.stack([reach, jnp.minimum(1.0, 2.0 * reach)]) * 2.0**-12.5
        unit[c] = jnp.maximum(units, 1e-30).astype(BF).astype(F32)

    def code(v, u):
        t = v * (1.0 / u)
        t = t * t
        t = t * t
        t = t * t
        return jnp.where(v < 0.0, -t, t)

    def decode(ref):
        y = ref[...].astype(F32)
        size = jnp.exp(0.125 * jnp.log(jnp.abs(y))) * y_unit(ref)
        return jnp.where(y < 0.0, -size, size)

    def y_unit(ref):
        return ref[:, :, WIDE - 1 : WIDE].astype(F32)

    def stack(cs, g, far):
        own = [firsts[c][2] if g == 0 else firsts[c][0] for c in cs]
        out = s2 if g else s1
        if far:
            for c in cs:
                raw_block(c, g, x).wait_recv()

        def rows_of(i):
            c = cs[i]
            return r1.at[c, g] if far else xr.at[c, own[i]]

        def matmul(n, slot):
            cols = pl.ds(pl.multiple_of(n * 256, 256), 256)
            lhs = jnp.concatenate([rows_of(i)[...].reshape(128, WIDE) for i in range(2)], axis=0)
            hil[slot] = jnp.dot(lhs, table[:, cols], preferred_element_type=F32)

        def combine(n, slot):
            for i, c in enumerate(cs):
                for half in range(2):
                    cols = pl.ds(pl.multiple_of(n * 256 + half * 128, 128), 128)
                    for b in range(4):
                        if far:
                            sums = [out[c, b, k, :, cols] for k in range(3)]
                        else:
                            sums = [jnp.zeros((8, 128), F32)] * 3
                        for d in range(4):
                            at = i * 128 + b * 32 + d * 8
                            hh = hil[slot, at : at + 8, half * 128 : half * 128 + 128]
                            xx = rows_of(i)[b, d, :, cols].astype(F32)
                            w = wn[c, 0, d] if far else ww[0, d]
                            q = wn[c, 1, d] if far else ww[1, d]
                            inverse = lax.rsqrt(xx * xx + hh * hh + q)
                            sums = [sums[0] + w * xx, sums[1] + xx * inverse, sums[2] + hh * inverse]
                        for k in range(3):
                            if far and g == 0:
                                u = unit[c, min(k, 1)]
                                y = code(sums[k], u)
                                if isinstance(n, int) and n == 7 and half == 1:
                                    lane = lax.broadcasted_iota(jnp.int32, (8, 128), 1)
                                    y = jnp.where(lane == 127, u, y)
                                coded[c, b, k, :, cols] = y.astype(BF)
                            else:
                                out[c, b, k, :, cols] = sums[k]

        matmul(0, 0)

        def tiles(m, carry):
            matmul(2 * m + 1, 1)
            combine(2 * m, 0)
            matmul(2 * m + 2, 0)
            combine(2 * m + 1, 1)
            return carry

        lax.fori_loop(0, 3, tiles, 0)
        matmul(7, 1)
        combine(6, 0)
        combine(7, 1)

    def second_order(c):
        v, q1, q2, v2 = seconds[c]
        return (v2, q1, q2, v)

    def sums_first(c, k):
        b = second_order(c)[k]
        return remote(coded.at[c, b], r2.at[c, b], b_s.at[c, k], b_r.at[c, k], at_first(c, firsts[c][2]))

    def sums_second(c, k):
        b = second_order(c)[k]
        return remote(s2.at[c, b], r3.at[c, k], c_s.at[c, k], c_r.at[c, k], at_second(c, seconds[c][1]))

    def sums_third(c):
        b = second_order(c)[2]
        return remote(s2.at[c, b], r4.at[c], d_s.at[c], d_r.at[c], at_second(c, seconds[c][2]))

    def stage_three(c):
        for k in range(2):
            b = second_order(c)[k]
            sums_first(c, k).wait_recv()
            s2[c, b] = s2[c, b] + decode(r2.at[c, b])
            sums_second(c, k).start()

    def stage_four(c):
        b = second_order(c)[2]
        sums_first(c, 2).wait_recv()
        sums_second(c, 0).wait_recv()
        s2[c, b] = s2[c, b] + decode(r2.at[c, b]) + r3[c, 0]
        sums_third(c).start()

    def finish(c):
        b = second_order(c)[3]
        sums_first(c, 3).wait_recv()
        sums_second(c, 1).wait_recv()
        sums_third(c).wait_recv()
        total = s2[c, b] + decode(r2.at[c, b]) + r3[c, 1] + r4[c]
        sums_ref[:, pl.ds(8 * c, 8), :] = total[:, :, :LAGS]

    stack((0, 1), 0, False)
    stack((2, 3), 0, False)
    for copy in weight_copies:
        copy.wait_recv()
    for c in range(4):
        scale_up(c)
    for cs in ((0, 1), (2, 3)):
        stack(cs, 0, True)
        for c in cs:
            for k in range(4):
                sums_first(c, k).start()
    for cs in ((0, 1), (2, 3)):
        stack(cs, 1, False)
        stack(cs, 1, True)
        for c in cs:
            stage_three(c)
    for c in range(4):
        stage_four(c)
    for c in range(4):
        finish(c)

    for copy in energy_copies + weight_copies:
        copy.wait_send()
    for c in range(4):
        for g in range(2):
            raw_block(c, g, x).wait_send()
        for k in range(4):
            sums_first(c, k).wait_send()
        for k in range(2):
            sums_second(c, k).wait_send()
        sums_third(c).wait_send()


def shards(correlations, mask, counts):
    lag_major = jnp.transpose(correlations, (2, 0, 1))
    vmem = pl.BlockSpec(memory_space=pltpu.VMEM)
    dma = pltpu.SemaphoreType.DMA
    linear_sum, phase_real, phase_imag = pl.pallas_call(
        kernel,
        out_shape=jax.ShapeDtypeStruct((3, 32, LAGS), F32),
        in_specs=[pl.BlockSpec(memory_space=pl.ANY), vmem],
        out_specs=vmem,
        scratch_shapes=[
            pltpu.VMEM((4, LAGS, 4, 128), BF),
            pltpu.VMEM((8192, 128), F32),
            pltpu.VMEM((4, 4, 4, 4, 8, WIDE), BF),
            pltpu.VMEM((4, 2, 4, 4, 8, WIDE), BF),
            pltpu.VMEM((WIDE, WIDE), BF),
            pltpu.VMEM((4, 4, 3, 8, WIDE), F32),
            pltpu.VMEM((4, 4, 3, 8, WIDE), F32),
            pltpu.VMEM((4, 4, 3, 8, WIDE), BF),
            pltpu.VMEM((4, 4, 3, 8, WIDE), BF),
            pltpu.VMEM((4, 2, 3, 8, WIDE), F32),
            pltpu.VMEM((4, 3, 8, WIDE), F32),
            pltpu.VMEM((8, 2, 8, 128), F32),
            pltpu.VMEM((3, 4, 8, 128), F32),
            pltpu.VMEM((4, 3, 4, 8, 128), F32),
            pltpu.VMEM((4, 2, 8, 128), F32),
            pltpu.VMEM((2, 256, 256), F32),
            pltpu.VMEM((8, 4096), F32),
            dma((4,)),
            dma((4, 2)), dma((4, 2)),
            dma((4, 4)), dma((4, 4)),
            dma((4, 2)), dma((4, 2)),
            dma((4,)), dma((4,)),
            dma((8,)), dma((8,)),
            dma((4,)), dma((4,)),
        ],
        compiler_params=pltpu.CompilerParams(
            collective_id=0, has_side_effects=True, vmem_limit_bytes=67043328
        ),
    )(lag_major, mask)
    divisor = jnp.maximum(counts.astype(F32), 1.0)[:, None]
    linear = linear_sum / divisor
    coherence = (phase_real * phase_real + phase_imag * phase_imag) / (divisor * divisor)
    return (linear * coherence, linear)


def solution(mesh):
    placed = (P("day", "pair", None), P("day", "pair"), P(("pair", "day")))
    return jax.shard_map(
        shards,
        mesh=mesh,
        in_specs=placed,
        out_specs=(P(("pair", "day"), None), P(("pair", "day"), None)),
        check_vma=False,
    )
```

```python
import jax
import jax.numpy as jnp
from jax import lax
from jax.experimental import pallas as pl
from jax.experimental.pallas import tpu as pltpu
from jax.sharding import PartitionSpec as P

BF = jnp.bfloat16
F32 = jnp.float32
MESH = pl.DeviceIdType.MESH
LAGS = 2001
WIDE = 2048


def alpha(v):
    return v + 1 - 2 * (v % 2)


def beta(v):
    return 3 - v


def hilbert_rows():
    u = lax.broadcasted_iota(jnp.int32, (8, 4096), 1)
    s = lax.broadcasted_iota(jnp.int32, (8, 4096), 0)
    t = jnp.where(u < 3840, u, u - 4096) - 1792 - s
    offset = jnp.where(t > LAGS // 2, t - LAGS, jnp.where(t < -(LAGS // 2), t + LAGS, t))
    phase_angle = jnp.pi * offset.astype(F32) / LAGS
    parity = 1.0 - 2.0 * (offset & 1).astype(F32)
    sine_safe = jnp.where(offset == 0, 1.0, jnp.sin(phase_angle))
    return jnp.where(offset == 0, 0.0, (jnp.cos(phase_angle) - parity) / (LAGS * sine_safe))


def kernel(x_hbm, mask_ref, counts_ref, sums_ref,
           slab, flat, xr, r1, table, s1, s2, coded, r2, r3, r4, en, ww, wn, unit, hil, rows_ref,
           in_sem, a_s, a_r, b_s, b_r, c_s, c_r, d_s, d_r, e_s, e_r, w_s, w_r):
    day = lax.axis_index("day")
    pair = lax.axis_index("pair")
    x = day // 4
    y = day % 4
    xa, xb, ya, yb = alpha(x), beta(x), alpha(y), beta(y)
    x2, y2 = (x + 2) % 4, (y + 2) % 4
    along_x_a, along_x_b = (x, xa, xb, x2), (x, xb, xa, x2)
    along_y_a, along_y_b = (y, ya, yb, y2), (y, yb, ya, y2)
    firsts = (along_x_a, along_x_b, along_y_a, along_y_b)
    seconds = (along_y_a, along_y_b, along_x_a, along_x_b)

    def at_first(c, v):
        return (v * 4 + y, pair) if c < 2 else (x * 4 + v, pair)

    def at_second(c, v):
        return (x * 4 + v, pair) if c < 2 else (v * 4 + y, pair)

    neighbours = [(xa * 4 + y, pair), (xb * 4 + y, pair), (x * 4 + ya, pair), (x * 4 + yb, pair)]
    peers = [(day, (pair + k) % 8) for k in range(1, 8)]

    def load_block(i, cb):
        cols = pl.ds(pl.multiple_of(cb * 128, 128), 128)
        return pltpu.make_async_copy(x_hbm.at[:, :, cols], slab.at[i], in_sem.at[i])

    order = (x2, xa, xb, x)
    loads = [load_block(i, cb) for i, cb in enumerate(order)]
    loads[0].start()

    barrier = pltpu.get_barrier_semaphore()
    for to in neighbours + peers:
        pl.semaphore_signal(barrier, inc=1, device_id=to, device_id_type=MESH)

    for i in range(3):
        flat[i, pl.ds(8000, 192), :] = jnp.zeros((192, 128), F32)
    rows_ref[...] = hilbert_rows()

    def remote(src, dst, send, recv, to):
        return pltpu.make_async_remote_copy(
            src_ref=src, dst_ref=dst, send_sem=send, recv_sem=recv, device_id=to, device_id_type=MESH
        )

    def raw_block(c, g, a):
        return remote(xr.at[c, a], r1.at[c, g], a_s.at[c, g], a_r.at[c, g], at_first(c, firsts[c][1]))

    def raw_piece(c, g, a, b):
        return remote(xr.at[c, a, b], r1.at[c, g, b], a_s.at[c, g], a_r.at[c, g], at_first(c, firsts[c][1]))

    totals = [jnp.zeros((8, 128), F32), jnp.zeros((8, 128), F32)]

    def widen(i):
        loads[i].wait()
        if i < 3:
            loads[i + 1].start()
        cols = pl.ds(pl.multiple_of(order[i] * 128, 128), 128)
        m4 = mask_ref[:, cols].astype(F32)
        m8 = jnp.concatenate([m4, m4], axis=0)
        rows = slab.at[i].reshape(4 * LAGS, 128)
        into = flat.at[max(i - 1, 0)]

        def step(j, acc):
            at = pl.ds(pl.multiple_of(j * 32, 32), 32)
            v = rows[at, :].astype(F32).reshape(4, 8, 128) * m8[None]
            into[at, :] = v.reshape(32, 128)
            return acc + jnp.sum(v * v, axis=0)

        squares = lax.fori_loop(0, 250, step, totals[0], unroll=10)
        last = rows[pl.ds(8000, 4), :].astype(F32) * m4
        into[pl.ds(8000, 4), :] = last
        totals[0] = squares + jnp.concatenate([last * last, jnp.zeros((4, 128), F32)], axis=0)
        totals[1] = totals[1] + m8

    def turn(i):
        cb = order[i]
        source = flat.at[max(i - 1, 0)]

        def step(j, carry):
            lags = pl.ds(pl.multiple_of(j * 128, 128), 128)
            for d in range(4):
                t = source[pl.ds(pl.multiple_of(j * 512, 512) + d, 128, stride=4), :]
                t = t.astype(BF).T.reshape(4, 4, 8, 128)
                for c in range(2):
                    xr[c, cb, :, d, :, lags] = t[:, c]
                for c in range(2, 4):
                    for q in range(4):
                        xr[c, q, cb, d, :, lags] = t[q, c]
            return carry

        lax.fori_loop(0, 16, step, 0, unroll=2)
        if i == 0:
            pl.semaphore_wait(barrier, len(neighbours) + len(peers))
            for c in range(2):
                raw_block(c, 0, x2).start()
        for c in range(2, 4):
            raw_piece(c, 0, y2, cb).start()

    widen(0)
    turn(0)
    widen(1)
    widen(2)
    widen(3)

    en[0, 0] = totals[0]
    en[0, 1] = totals[1]
    energy_copies = [
        remote(en.at[0], en.at[k], e_s.at[k], e_r.at[k], peers[k - 1]) for k in range(1, 8)
    ]
    for copy in energy_copies:
        copy.start()
    turn(1)
    turn(2)
    turn(3)

    def tabulate(j, carry):
        lo = pltpu.roll(rows_ref[...], j * 16, 1)
        hi = pltpu.roll(rows_ref[...], j * 16 + 8, 1)
        both = jnp.concatenate([lo, hi], axis=0).astype(BF)
        for a in range(8):
            table[pl.ds(pl.multiple_of(a * 256 + j * 16, 16), 16), :] = both[:, 256 * (7 - a) : 256 * (7 - a) + WIDE]
        return carry

    lax.fori_loop(0, 16, tabulate, 0)

    for copy in energy_copies:
        copy.wait_recv()
    total = jnp.sum(en[:, 0], axis=0)
    pairs_used = jnp.sum(en[:, 1], axis=0)
    energy = jnp.sum(total[:4] + total[4:], axis=1, keepdims=True)
    pairs_used = jnp.sum(pairs_used[:4], axis=1, keepdims=True)
    level = energy / (LAGS * jnp.maximum(pairs_used, 1.0)) + 0.1
    weight = lax.rsqrt(level)
    reach = weight * jnp.sqrt(energy)
    for d in range(4):
        ww[0, d] = jnp.broadcast_to(weight[d : d + 1], (8, 128))
        ww[1, d] = jnp.broadcast_to(0.25 * level[d : d + 1], (8, 128))
        ww[2, d] = jnp.broadcast_to(reach[d : d + 1], (8, 128))
    weight_copies = [remote(ww, wn.at[k], w_s.at[k], w_r.at[k], neighbours[k]) for k in range(4)]
    for copy in weight_copies:
        copy.start()
    for c in range(4):
        raw_block(c, 1, firsts[c][1]).start()

    def scale_up(c):
        reach = jnp.maximum(jnp.max(ww[2], axis=0), jnp.max(wn[c, 2], axis=0))
        units = jnp.stack([reach, jnp.minimum(1.0, 2.0 * reach)]) * 2.0**-12.5
        unit[c] = jnp.maximum(units, 1e-30).astype(BF).astype(F32)

    def code(v, u):
        t = v * (1.0 / u)
        t = t * t
        t = t * t
        t = t * t
        return jnp.where(v < 0.0, -t, t)

    def decode(ref):
        y = ref[...].astype(F32)
        size = jnp.exp(0.125 * jnp.log(jnp.abs(y))) * y_unit(ref)
        return jnp.where(y < 0.0, -size, size)

    def y_unit(ref):
        return ref[:, :, WIDE - 1 : WIDE].astype(F32)

    def second_order(c):
        v, q1, q2, v2 = seconds[c]
        return (v2, q1, q2, v)

    def tile_sums(parts, slot, half, cols, sums):
        for at, raw, wq in parts:
            for d in range(4):
                hh = hil[slot, at + 8 * d : at + 8 * d + 8, half * 128 : half * 128 + 128]
                xx = raw[d, :, cols].astype(F32)
                inverse = lax.rsqrt(xx * xx + hh * hh + wq[1, d])
                sums = [sums[0] + wq[0, d] * xx, sums[1] + xx * inverse, sums[2] + hh * inverse]
        return sums

    def halves(n):
        for half in range(2):
            yield half, pl.ds(pl.multiple_of(n * 256 + half * 128, 128), 128)

    class FirstSums:
        def __init__(self, cs, far):
            self.cs, self.far = cs, far

        def before(self):
            if self.far:
                if self.cs[0] == 0:
                    for copy in weight_copies:
                        copy.wait_recv()
                    for c in range(4):
                        scale_up(c)
                for c in self.cs:
                    raw_block(c, 0, x).wait_recv()

        def rows(self, c):
            return r1.at[c, 0] if self.far else xr.at[c, firsts[c][2]]

        def left(self):
            return [self.rows(c)[...].reshape(128, WIDE) for c in self.cs]

        def combine(self, n, slot):
            for i, c in enumerate(self.cs):
                wq = wn.at[c] if self.far else ww
                for half, cols in halves(n):
                    for b in range(4):
                        sums = [s1[c, b, k, :, cols] for k in range(3)] if self.far else [jnp.zeros((8, 128), F32)] * 3
                        sums = tile_sums([(i * 128 + b * 32, self.rows(c).at[b], wq)], slot, half, cols, sums)
                        for k in range(3):
                            if not self.far:
                                s1[c, b, k, :, cols] = sums[k]
                                continue
                            u = unit[c, min(k, 1)]
                            y = code(sums[k], u)
                            if isinstance(n, int) and n == 7 and half == 1:
                                lane = lax.broadcasted_iota(jnp.int32, (8, 128), 1)
                                y = jnp.where(lane == 127, u, y)
                            coded[c, b, k, :, cols] = y.astype(BF)

        def after(self):
            if self.far:
                for c in self.cs:
                    for k in range(4):
                        sums_first(c, k).start()

    class SecondSums:
        def __init__(self, k):
            self.k = k

        def before(self):
            if self.k == 0:
                for c in range(4):
                    raw_block(c, 1, x).wait_recv()

        def rows(self, c):
            b = second_order(c)[self.k]
            return xr.at[c, firsts[c][0], b], r1.at[c, 1, b]

        def left(self):
            return [r[...].reshape(32, WIDE) for c in range(4) for r in self.rows(c)]

        def combine(self, n, slot):
            for c in range(4):
                own, far = self.rows(c)
                for half, cols in halves(n):
                    parts = [(c * 64, own, ww), (c * 64 + 32, far, wn.at[c])]
                    sums = tile_sums(parts, slot, half, cols, [jnp.zeros((8, 128), F32)] * 3)
                    for k in range(3):
                        s2[c, self.k, k, :, cols] = sums[k]

        def after(self):
            for c in range(4):
                (stage_three, stage_three, stage_four, finish)[self.k](c, self.k)

    def matmul(job, n, slot):
        cols = pl.ds(pl.multiple_of(n * 256, 256), 256)
        lhs = jnp.concatenate(job.left(), axis=0)
        hil[slot] = jnp.dot(lhs, table[:, cols], preferred_element_type=F32)

    def sums_first(c, k):
        b = second_order(c)[k]
        return remote(coded.at[c, b], r2.at[c, k], b_s.at[c, k], b_r.at[c, k], at_first(c, firsts[c][2]))

    def sums_second(c, k):
        return remote(s2.at[c, k], r3.at[c, k], c_s.at[c, k], c_r.at[c, k], at_second(c, seconds[c][1]))

    def sums_third(c):
        return remote(s2.at[c, 2], r4.at[c], d_s.at[c], d_r.at[c], at_second(c, seconds[c][2]))

    def stage_three(c, k):
        sums_first(c, k).wait_recv()
        s2[c, k] = s2[c, k] + decode(r2.at[c, k])
        sums_second(c, k).start()

    def stage_four(c, k):
        sums_first(c, 2).wait_recv()
        sums_second(c, 0).wait_recv()
        s2[c, 2] = s2[c, 2] + decode(r2.at[c, 2]) + r3[c, 0]
        sums_third(c).start()

    def finish(c, k):
        sums_first(c, 3).wait_recv()
        sums_second(c, 1).wait_recv()
        sums_third(c).wait_recv()
        total = s2[c, 3] + decode(r2.at[c, 3]) + r3[c, 1] + r4[c]
        n = counts_column[8 * c : 8 * c + 8]
        sums_ref[0, pl.ds(8 * c, 8), :] = (total[0] / n)[:, :LAGS]
        sums_ref[1, pl.ds(8 * c, 8), :] = ((total[1] * total[1] + total[2] * total[2]) / (n * n))[:, :LAGS]

    counts = jnp.broadcast_to(jnp.maximum(counts_ref[...].astype(F32), 1.0), (32, 32))
    across = lax.broadcasted_iota(jnp.int32, (32, 32), 0) == lax.broadcasted_iota(jnp.int32, (32, 32), 1)
    counts_column = jnp.sum(jnp.where(across, counts, 0.0), axis=1, keepdims=True)

    jobs = [FirstSums(cs, far) for far in (False, True) for cs in ((0, 1), (2, 3))]
    jobs += [SecondSums(k) for k in range(4)]
    matmul(jobs[0], 0, 0)
    for job, following in zip(jobs, jobs[1:] + [None]):

        def tiles(m, carry, job=job):
            matmul(job, 2 * m + 1, 1)
            job.combine(2 * m, 0)
            matmul(job, 2 * m + 2, 0)
            job.combine(2 * m + 1, 1)
            return carry

        lax.fori_loop(0, 3, tiles, 0)
        if following:
            following.before()
        matmul(job, 7, 1)
        job.combine(6, 0)
        if following:
            matmul(following, 0, 0)
        job.combine(7, 1)
        job.after()

    for copy in energy_copies + weight_copies:
        copy.wait_send()
    for c in range(4):
        for g in range(2):
            raw_block(c, g, x).wait_send()
        for k in range(4):
            sums_first(c, k).wait_send()
        for k in range(2):
            sums_second(c, k).wait_send()
        sums_third(c).wait_send()


def shards(correlations, mask, counts):
    lag_major = jnp.transpose(correlations, (2, 0, 1))
    vmem = pl.BlockSpec(memory_space=pltpu.VMEM)
    dma = pltpu.SemaphoreType.DMA
    linear, coherence = pl.pallas_call(
        kernel,
        out_shape=jax.ShapeDtypeStruct((2, 32, LAGS), F32),
        in_specs=[pl.BlockSpec(memory_space=pl.ANY), vmem, vmem],
        out_specs=vmem,
        scratch_shapes=[
            pltpu.VMEM((4, LAGS, 4, 128), BF),
            pltpu.VMEM((3, 8192, 128), F32),
            pltpu.VMEM((4, 4, 4, 4, 8, WIDE), BF),
            pltpu.VMEM((4, 2, 4, 4, 8, WIDE), BF),
            pltpu.VMEM((WIDE, WIDE), BF),
            pltpu.VMEM((4, 4, 3, 8, WIDE), F32),
            pltpu.VMEM((4, 4, 3, 8, WIDE), F32),
            pltpu.VMEM((4, 4, 3, 8, WIDE), BF),
            pltpu.VMEM((4, 4, 3, 8, WIDE), BF),
            pltpu.VMEM((4, 2, 3, 8, WIDE), F32),
            pltpu.VMEM((4, 3, 8, WIDE), F32),
            pltpu.VMEM((8, 2, 8, 128), F32),
            pltpu.VMEM((3, 4, 8, 128), F32),
            pltpu.VMEM((4, 3, 4, 8, 128), F32),
            pltpu.VMEM((4, 2, 8, 128), F32),
            pltpu.VMEM((2, 256, 256), F32),
            pltpu.VMEM((8, 4096), F32),
            dma((4,)),
            dma((4, 2)), dma((4, 2)),
            dma((4, 4)), dma((4, 4)),
            dma((4, 2)), dma((4, 2)),
            dma((4,)), dma((4,)),
            dma((8,)), dma((8,)),
            dma((4,)), dma((4,)),
        ],
        compiler_params=pltpu.CompilerParams(
            collective_id=0, has_side_effects=True, vmem_limit_bytes=58 * 2**20
        ),
    )(lag_major, mask, counts[None])
    return (linear * coherence, linear)


def solution(mesh):
    placed = (P("day", "pair", None), P("day", "pair"), P(("pair", "day")))
    return jax.shard_map(
        shards,
        mesh=mesh,
        in_specs=placed,
        out_specs=(P(("pair", "day"), None), P(("pair", "day"), None)),
        check_vma=False,
    )
```

```python
import jax
import jax.numpy as jnp
from jax import lax
from jax.experimental import pallas as pl
from jax.experimental.pallas import tpu as pltpu
from jax.sharding import PartitionSpec as P

BF = jnp.bfloat16
F32 = jnp.float32
MESH = pl.DeviceIdType.MESH
LAGS = 2001
WIDE = 2048
EARLY = 3


def alpha(v):
    return v + 1 - 2 * (v % 2)


def beta(v):
    return 3 - v


def hilbert_rows():
    u = lax.broadcasted_iota(jnp.int32, (8, 4096), 1)
    s = lax.broadcasted_iota(jnp.int32, (8, 4096), 0)
    t = jnp.where(u < 3840, u, u - 4096) - 1792 - s
    offset = jnp.where(t > LAGS // 2, t - LAGS, jnp.where(t < -(LAGS // 2), t + LAGS, t))
    phase_angle = jnp.pi * offset.astype(F32) / LAGS
    parity = 1.0 - 2.0 * (offset & 1).astype(F32)
    sine_safe = jnp.where(offset == 0, 1.0, jnp.sin(phase_angle))
    return jnp.where(offset == 0, 0.0, (jnp.cos(phase_angle) - parity) / (LAGS * sine_safe))


def kernel(x_hbm, mask_ref, counts_ref, sums_ref,
           slab, flat, xr, r1, table, s1, s2, coded, r2, third, r3, r4, en, ww, wn, unit, hil, rows_ref,
           in_sem, a_s, a_r, g_s, g_r, b_s, b_r, c_s, c_r, d_s, d_r, e_s, e_r, w_s, w_r):
    day = lax.axis_index("day")
    pair = lax.axis_index("pair")
    x = day // 4
    y = day % 4
    xa, xb, ya, yb = alpha(x), beta(x), alpha(y), beta(y)
    x2, y2 = (x + 2) % 4, (y + 2) % 4
    along_x_a, along_x_b = (x, xa, xb, x2), (x, xb, xa, x2)
    along_y_a, along_y_b = (y, ya, yb, y2), (y, yb, ya, y2)
    firsts = (along_x_a, along_x_b, along_y_a, along_y_b)
    seconds = (along_y_a, along_y_b, along_x_a, along_x_b)

    def at_first(c, v):
        return (v * 4 + y, pair) if c < 2 else (x * 4 + v, pair)

    def at_second(c, v):
        return (x * 4 + v, pair) if c < 2 else (v * 4 + y, pair)

    neighbours = [(xa * 4 + y, pair), (xb * 4 + y, pair), (x * 4 + ya, pair), (x * 4 + yb, pair)]
    peers = [(day, (pair + k) % 8) for k in range(1, 8)]

    def load(i, start, size, sem):
        cols = pl.ds(pl.multiple_of(order[i] * 128, 128), 128)
        lags = pl.ds(start, size)
        return pltpu.make_async_copy(x_hbm.at[lags, :, cols], slab.at[i % 2, lags], in_sem.at[sem])

    order = (x2, xa, xb, x)
    first_loads = [load(0, 512 * q, min(512, LAGS - 512 * q), q) for q in range(4)]
    loads = [None] + [load(i, 0, LAGS, 3 + i) for i in range(1, 4)]
    for copy in first_loads + [loads[1]]:
        copy.start()

    barrier = pltpu.get_barrier_semaphore()
    for to in neighbours + peers:
        pl.semaphore_signal(barrier, inc=1, device_id=to, device_id_type=MESH)

    for i in range(2):
        slab[i, pl.ds(LAGS, WIDE - LAGS)] = jnp.zeros((WIDE - LAGS, 4, 128), BF)
    rows_ref[...] = hilbert_rows()

    def remote(src, dst, send, recv, to):
        return pltpu.make_async_remote_copy(
            src_ref=src, dst_ref=dst, send_sem=send, recv_sem=recv, device_id=to, device_id_type=MESH
        )

    def raw_block(c, a):
        return remote(xr.at[c, a], r1.at[c, 0], a_s.at[c], a_r.at[c], at_first(c, firsts[c][1]))

    def raw_piece(c, a, b):
        return remote(xr.at[c, a, b], r1.at[c, 0, b], a_s.at[c], a_r.at[c], at_first(c, firsts[c][1]))

    def second_order(c):
        v, q1, q2, v2 = seconds[c]
        return (v2, q1, q2, v)

    def raw_second(c, k):
        source = xr.at[c, firsts[c][1], second_order(c)[k]]
        return remote(source, r1.at[c, 1, k], g_s.at[c, k], g_r.at[c, k], at_first(c, firsts[c][1]))

    masks = []
    for cb in order:
        m4 = mask_ref[:, pl.ds(pl.multiple_of(cb * 128, 128), 128)].astype(F32)
        masks.append(jnp.concatenate([m4, m4], axis=0))

    def widen(i, j, acc):
        rows = slab.at[i % 2].reshape(4 * WIDE, 128)
        for r in range(16):
            at = pl.ds(pl.multiple_of(j * 512, 512) + 32 * r, 32)
            v = rows[at, :].astype(F32).reshape(4, 8, 128) * masks[i][None]
            flat[max(i - 1, 0), at, :] = v.reshape(32, 128)
            acc = acc + jnp.sum(v * v, axis=0)
        return acc

    def turn(i, j):
        lags = pl.ds(pl.multiple_of(j * 128, 128), 128)
        for d in range(4):
            t = flat[max(i - 1, 0), pl.ds(pl.multiple_of(j * 512, 512) + d, 128, stride=4), :]
            t = t.astype(BF).T.reshape(4, 4, 8, 128)
            for c in range(2):
                xr[c, order[i], :, d, :, lags] = t[:, c]
            for c in range(2, 4):
                for q in range(4):
                    xr[c, q, order[i], d, :, lags] = t[q, c]

    def send_raw(i):
        if i == 0:
            pl.semaphore_wait(barrier, len(neighbours) + len(peers))
            for c in range(2):
                raw_block(c, x2).start()
        for c in range(2, 4):
            raw_piece(c, y2, order[i]).start()
            if i == 0:
                raw_second(c, 0).start()

    def tabulate(j, carry):
        lo = pltpu.roll(rows_ref[...], j * 16, 1)
        hi = pltpu.roll(rows_ref[...], j * 16 + 8, 1)
        both = jnp.concatenate([lo, hi], axis=0).astype(BF)
        for a in range(8):
            table[pl.ds(pl.multiple_of(a * 256 + j * 16, 16), 16), :] = both[:, 256 * (7 - a) : 256 * (7 - a) + WIDE]
        return carry

    lax.fori_loop(0, EARLY, tabulate, 0)

    squares = jnp.zeros((8, 128), F32)
    for q in range(4):
        first_loads[q].wait()
        squares = lax.fori_loop(4 * q, 4 * q + 4, lambda j, acc: widen(0, j, acc), squares)
    def turn_all(i):
        def step(j, carry):
            turn(i, j)
            return carry

        lax.fori_loop(0, 16, step, 0, unroll=2)
        send_raw(i)

    turn_all(0)
    for i in range(1, 4):
        loads[i].wait()
        if i < 3:
            loads[i + 1].start()
        squares = lax.fori_loop(0, 16, lambda j, acc, i=i: widen(i, j, acc), squares)

    en[0, 0] = squares
    en[0, 1] = masks[0] + masks[1] + masks[2] + masks[3]
    energy_copies = [
        remote(en.at[0], en.at[k], e_s.at[k], e_r.at[k], peers[k - 1]) for k in range(1, 8)
    ]
    for copy in energy_copies:
        copy.start()

    for i in range(1, 4):
        turn_all(i)

    lax.fori_loop(EARLY, 16, tabulate, 0)

    for copy in energy_copies:
        copy.wait_recv()
    total = jnp.sum(en[:, 0], axis=0)
    pairs_used = jnp.sum(en[:, 1], axis=0)
    energy = jnp.sum(total[:4] + total[4:], axis=1, keepdims=True)
    pairs_used = jnp.sum(pairs_used[:4], axis=1, keepdims=True)
    level = energy / (LAGS * jnp.maximum(pairs_used, 1.0)) + 0.1
    weight = lax.rsqrt(level)
    reach = weight * jnp.sqrt(energy)
    for d in range(4):
        ww[0, d] = jnp.broadcast_to(weight[d : d + 1], (8, 128))
        ww[1, d] = jnp.broadcast_to(0.25 * level[d : d + 1], (8, 128))
        ww[2, d] = jnp.broadcast_to(reach[d : d + 1], (8, 128))
    weight_copies = [remote(ww, wn.at[k], w_s.at[k], w_r.at[k], neighbours[k]) for k in range(4)]
    for copy in weight_copies:
        copy.start()
    for k in range(4):
        for c in range(4 if k else 2):
            raw_second(c, k).start()

    def scale_up(c):
        reach = jnp.maximum(jnp.max(ww[2], axis=0), jnp.max(wn[c, 2], axis=0))
        units = jnp.stack([reach, jnp.minimum(1.0, 2.0 * reach)]) * 2.0**-9.6
        unit[c] = jnp.maximum(units, 1e-30).astype(BF).astype(F32)

    def code(v, u):
        t = v * (1.0 / u)
        t2 = t * t
        t4 = t2 * t2
        t = t4 * t4 * t2
        return jnp.where(v < 0.0, -t, t)

    def root(y, last, power):
        units = last[..., 127:128]
        size = jnp.exp((1.0 / power) * jnp.log(jnp.abs(y))) * units
        return jnp.where(y < 0.0, -size, size)

    def decode(ref):
        y = ref[...].astype(F32)
        return root(y, y[:, :, WIDE - 128 :], 10)

    def code_whole(v):
        largest = jnp.max(jnp.max(jnp.abs(v), axis=2, keepdims=True), axis=1, keepdims=True)
        u = (jnp.maximum(largest, 1e-30) * 2.0**-10.4).astype(BF).astype(F32)
        t = v * (1.0 / u)
        t2 = t * t
        t4 = t2 * t2
        t = t4 * t4 * t4
        lane = lax.broadcasted_iota(jnp.int32, (3, 8, WIDE), 2)
        return jnp.where(lane == WIDE - 1, u, jnp.where(v < 0.0, -t, t)).astype(BF)

    def decode_whole(ref):
        y = ref[...].astype(F32)
        return root(y, y[:, :, WIDE - 128 :], 12)

    def tile_sums(parts, slot, half, cols, sums):
        for at, raw, wq in parts:
            for d in range(4):
                hh = hil[slot, at + 8 * d : at + 8 * d + 8, half * 128 : half * 128 + 128]
                xx = raw[d, :, cols].astype(F32)
                inverse = lax.rsqrt(xx * xx + hh * hh + wq[1, d])
                sums = [sums[0] + wq[0, d] * xx, sums[1] + xx * inverse, sums[2] + hh * inverse]
        return sums

    def halves(n):
        for half in range(2):
            yield half, pl.ds(pl.multiple_of(n * 256 + half * 128, 128), 128)

    class FirstSums:
        def __init__(self, cs, far):
            self.cs, self.far = cs, far

        def before(self):
            if self.far:
                for c in self.cs:
                    weight_copies[c].wait_recv()
                    scale_up(c)
                    raw_block(c, x).wait_recv()

        def rows(self, c):
            return r1.at[c, 0] if self.far else xr.at[c, firsts[c][2]]

        def left(self):
            return [self.rows(c)[...].reshape(128, WIDE) for c in self.cs]

        def combine(self, n, slot):
            for i, c in enumerate(self.cs):
                wq = wn.at[c] if self.far else ww
                for half, cols in halves(n):
                    for b in range(4):
                        sums = [s1[c, b, k, :, cols] for k in range(3)] if self.far else [jnp.zeros((8, 128), F32)] * 3
                        sums = tile_sums([(i * 128 + b * 32, self.rows(c).at[b], wq)], slot, half, cols, sums)
                        for k in range(3):
                            if not self.far:
                                s1[c, b, k, :, cols] = sums[k]
                                continue
                            u = unit[c, min(k, 1)]
                            y = code(sums[k], u)
                            if isinstance(n, int) and n == 7 and half == 1:
                                lane = lax.broadcasted_iota(jnp.int32, (8, 128), 1)
                                y = jnp.where(lane == 127, u, y)
                            coded[c, b, k, :, cols] = y.astype(BF)

        def after(self):
            if self.far:
                for c in self.cs:
                    for k in range(2):
                        sums_first(c, k).start()

    class SecondSums:
        def __init__(self, k):
            self.k = k

        def before(self):
            for c in range(4):
                raw_second(c, self.k).wait_recv()
                if self.k == 3:
                    sums_first(c, self.k).wait_recv()

        def rows(self, c):
            b = second_order(c)[self.k]
            return xr.at[c, firsts[c][0], b], r1.at[c, 1, self.k]

        def left(self):
            return [r[...].reshape(32, WIDE) for c in range(4) for r in self.rows(c)]

        def combine(self, n, slot):
            for c in range(4):
                own, far = self.rows(c)
                for half, cols in halves(n):
                    parts = [(c * 64, own, ww), (c * 64 + 32, far, wn.at[c])]
                    if self.k == 3:
                        last = pl.ds(WIDE - 128, 128)
                        sums = [root(r2[c, self.k, k, :, cols].astype(F32), r2[c, self.k, k, :, last].astype(F32), 10) for k in range(3)]
                    else:
                        sums = [jnp.zeros((8, 128), F32)] * 3
                    sums = tile_sums(parts, slot, half, cols, sums)
                    for k in range(3):
                        s2[c, self.k, k, :, cols] = sums[k]

        def after(self):
            for c in range(4):
                (stage_three, stage_three, stage_four, finish)[self.k](c, self.k)
            if self.k == 0:
                for k in range(2, 4):
                    for c in range(4):
                        sums_first(c, k).start()

    def matmul(job, n, slot):
        cols = pl.ds(pl.multiple_of(n * 256, 256), 256)
        lhs = jnp.concatenate(job.left(), axis=0)
        hil[slot] = jnp.dot(lhs, table[:, cols], preferred_element_type=F32)

    def sums_first(c, k):
        b = second_order(c)[k]
        return remote(coded.at[c, b], r2.at[c, k], b_s.at[c, k], b_r.at[c, k], at_first(c, firsts[c][2]))

    def sums_second(c, k):
        return remote(third.at[c, k], r3.at[c, k], c_s.at[c, k], c_r.at[c, k], at_second(c, seconds[c][1]))

    def sums_third(c):
        return remote(third.at[c, 2], r4.at[c], d_s.at[c], d_r.at[c], at_second(c, seconds[c][2]))

    def stage_three(c, k):
        sums_first(c, k).wait_recv()
        third[c, k] = code_whole(s2[c, k] + decode(r2.at[c, k]))
        sums_second(c, k).start()

    def stage_four(c, k):
        sums_first(c, 2).wait_recv()
        sums_second(c, 0).wait_recv()
        third[c, 2] = code_whole(s2[c, 2] + decode(r2.at[c, 2]) + decode_whole(r3.at[c, 0]))
        sums_third(c).start()

    def finish(c, k):
        sums_second(c, 1).wait_recv()
        sums_third(c).wait_recv()
        total = s2[c, 3] + decode_whole(r3.at[c, 1]) + decode_whole(r4.at[c])
        n = counts_column[8 * c : 8 * c + 8]
        sums_ref[0, pl.ds(8 * c, 8), :] = (total[0] / n)[:, :LAGS]
        sums_ref[1, pl.ds(8 * c, 8), :] = ((total[1] * total[1] + total[2] * total[2]) / (n * n))[:, :LAGS]

    counts = jnp.broadcast_to(jnp.maximum(counts_ref[...].astype(F32), 1.0), (32, 32))
    across = lax.broadcasted_iota(jnp.int32, (32, 32), 0) == lax.broadcasted_iota(jnp.int32, (32, 32), 1)
    counts_column = jnp.sum(jnp.where(across, counts, 0.0), axis=1, keepdims=True)

    jobs = [FirstSums(cs, far) for far in (False, True) for cs in ((0, 1), (2, 3))]
    jobs += [SecondSums(k) for k in range(4)]
    matmul(jobs[0], 0, 0)
    for job, following in zip(jobs, jobs[1:] + [None]):

        def tiles(m, carry, job=job):
            matmul(job, 2 * m + 1, 1)
            job.combine(2 * m, 0)
            matmul(job, 2 * m + 2, 0)
            job.combine(2 * m + 1, 1)
            return carry

        lax.fori_loop(0, 3, tiles, 0)
        if following:
            following.before()
        matmul(job, 7, 1)
        job.combine(6, 0)
        if following:
            matmul(following, 0, 0)
        job.combine(7, 1)
        job.after()

    for copy in energy_copies + weight_copies:
        copy.wait_send()
    for c in range(4):
        raw_block(c, x).wait_send()
        for k in range(4):
            raw_second(c, k).wait_send()
            sums_first(c, k).wait_send()
        for k in range(2):
            sums_second(c, k).wait_send()
        sums_third(c).wait_send()


def shards(correlations, mask, counts):
    lag_major = jnp.transpose(correlations, (2, 0, 1))
    vmem = pl.BlockSpec(memory_space=pltpu.VMEM)
    dma = pltpu.SemaphoreType.DMA
    linear, coherence = pl.pallas_call(
        kernel,
        out_shape=pltpu.VMEM((2, 32, LAGS), F32),
        in_specs=[pl.BlockSpec(memory_space=pl.ANY), vmem, vmem],
        out_specs=vmem,
        scratch_shapes=[
            pltpu.VMEM((2, WIDE, 4, 128), BF),
            pltpu.VMEM((3, 8192, 128), F32),
            pltpu.VMEM((4, 4, 4, 4, 8, WIDE), BF),
            pltpu.VMEM((4, 2, 4, 4, 8, WIDE), BF),
            pltpu.VMEM((WIDE, WIDE), BF),
            pltpu.VMEM((4, 4, 3, 8, WIDE), F32),
            pltpu.VMEM((4, 4, 3, 8, WIDE), F32),
            pltpu.VMEM((4, 4, 3, 8, WIDE), BF),
            pltpu.VMEM((4, 4, 3, 8, WIDE), BF),
            pltpu.VMEM((4, 3, 3, 8, WIDE), BF),
            pltpu.VMEM((4, 2, 3, 8, WIDE), BF),
            pltpu.VMEM((4, 3, 8, WIDE), BF),
            pltpu.VMEM((8, 2, 8, 128), F32),
            pltpu.VMEM((3, 4, 8, 128), F32),
            pltpu.VMEM((4, 3, 4, 8, 128), F32),
            pltpu.VMEM((4, 2, 8, 128), F32),
            pltpu.VMEM((2, 256, 256), F32),
            pltpu.VMEM((8, 4096), F32),
            dma((7,)),
            dma((4,)), dma((4,)),
            dma((4, 4)), dma((4, 4)),
            dma((4, 4)), dma((4, 4)),
            dma((4, 2)), dma((4, 2)),
            dma((4,)), dma((4,)),
            dma((8,)), dma((8,)),
            dma((4,)), dma((4,)),
        ],
        compiler_params=pltpu.CompilerParams(
            collective_id=0, has_side_effects=True, vmem_limit_bytes=58 * 2**20
        ),
    )(lag_major, mask, counts[None])
    return (linear * coherence, linear)


def solution(mesh):
    placed = (P("day", "pair", None), P("day", "pair"), P(("pair", "day")))
    return jax.shard_map(
        shards,
        mesh=mesh,
        in_specs=placed,
        out_specs=(P(("pair", "day"), None), P(("pair", "day"), None)),
        check_vma=False,
    )
```

```python
import jax
import jax.numpy as jnp
from jax import lax
from jax.experimental import pallas as pl
from jax.experimental.pallas import tpu as pltpu
from jax.sharding import PartitionSpec as P

BF = jnp.bfloat16
F32 = jnp.float32
MESH = pl.DeviceIdType.MESH
LAGS = 2001
WIDE = 2048
EARLY = 3


def alpha(v):
    return v + 1 - 2 * (v % 2)


def beta(v):
    return 3 - v


def hilbert_rows():
    u = lax.broadcasted_iota(jnp.int32, (8, 4096), 1)
    s = lax.broadcasted_iota(jnp.int32, (8, 4096), 0)
    t = jnp.where(u < 3840, u, u - 4096) - 1792 - s
    offset = jnp.where(t > LAGS // 2, t - LAGS, jnp.where(t < -(LAGS // 2), t + LAGS, t))
    phase_angle = jnp.pi * offset.astype(F32) / LAGS
    parity = 1.0 - 2.0 * (offset & 1).astype(F32)
    sine_safe = jnp.where(offset == 0, 1.0, jnp.sin(phase_angle))
    return jnp.where(offset == 0, 0.0, (jnp.cos(phase_angle) - parity) / (LAGS * sine_safe))


def kernel(x_hbm, mask_ref, counts_ref, sums_ref,
           slab, flat, xr, r1, table, s1, s2, coded, r2, third, r3, r4, en, ww, wn, unit, hil, rows_ref,
           in_sem, a_s, a_r, g_s, g_r, b_s, b_r, c_s, c_r, d_s, d_r, e_s, e_r, w_s, w_r):
    day = lax.axis_index("day")
    pair = lax.axis_index("pair")
    x = day // 4
    y = day % 4
    xa, xb, ya, yb = alpha(x), beta(x), alpha(y), beta(y)
    x2, y2 = (x + 2) % 4, (y + 2) % 4
    along_x_a, along_x_b = (x, xa, xb, x2), (x, xb, xa, x2)
    along_y_a, along_y_b = (y, ya, yb, y2), (y, yb, ya, y2)
    firsts = (along_x_a, along_x_b, along_y_a, along_y_b)
    seconds = (along_y_a, along_y_b, along_x_a, along_x_b)

    def at_first(c, v):
        return (v * 4 + y, pair) if c < 2 else (x * 4 + v, pair)

    def at_second(c, v):
        return (x * 4 + v, pair) if c < 2 else (v * 4 + y, pair)

    neighbours = [(xa * 4 + y, pair), (xb * 4 + y, pair), (x * 4 + ya, pair), (x * 4 + yb, pair)]
    peers = [(day, (pair + k) % 8) for k in range(1, 8)]

    def load(i, start, size, sem):
        cols = pl.ds(pl.multiple_of(order[i] * 128, 128), 128)
        lags = pl.ds(start, size)
        return pltpu.make_async_copy(x_hbm.at[lags, :, cols], slab.at[i % 2, lags], in_sem.at[sem])

    order = (x2, xa, xb, x)
    first_loads = [load(0, 512 * q, min(512, LAGS - 512 * q), q) for q in range(4)]
    loads = [None] + [load(i, 0, LAGS, 3 + i) for i in range(1, 4)]
    for copy in first_loads + [loads[1]]:
        copy.start()

    barrier = pltpu.get_barrier_semaphore()
    for to in neighbours + peers:
        pl.semaphore_signal(barrier, inc=1, device_id=to, device_id_type=MESH)

    for i in range(2):
        slab[i, pl.ds(LAGS, WIDE - LAGS)] = jnp.zeros((WIDE - LAGS, 4, 128), BF)
    rows_ref[...] = hilbert_rows()

    def remote(src, dst, send, recv, to):
        return pltpu.make_async_remote_copy(
            src_ref=src, dst_ref=dst, send_sem=send, recv_sem=recv, device_id=to, device_id_type=MESH
        )

    def raw_block(c, a):
        return remote(xr.at[c, a], r1.at[c, 0], a_s.at[c], a_r.at[c], at_first(c, firsts[c][1]))

    def raw_piece(c, a, b):
        return remote(xr.at[c, a, b], r1.at[c, 0, b], a_s.at[c], a_r.at[c], at_first(c, firsts[c][1]))

    def second_order(c):
        v, q1, q2, v2 = seconds[c]
        return (v2, q1, q2, v)

    def raw_second(c, k):
        source = xr.at[c, firsts[c][1], second_order(c)[k]]
        return remote(source, r1.at[c, 1, k], g_s.at[c, k], g_r.at[c, k], at_first(c, firsts[c][1]))

    masks = []
    for cb in order:
        m4 = mask_ref[:, pl.ds(pl.multiple_of(cb * 128, 128), 128)].astype(F32)
        masks.append(jnp.concatenate([m4, m4], axis=0))

    def widen(i, j, acc):
        rows = slab.at[i % 2].reshape(4 * WIDE, 128)
        narrow = jnp.concatenate([masks[i]] * 4, axis=0).astype(BF)
        for r in range(16):
            at = pl.ds(pl.multiple_of(j * 512, 512) + 32 * r, 32)
            v = (rows[at, :] * narrow).astype(F32).reshape(4, 8, 128)
            flat[max(i - 1, 0), at, :] = v.reshape(32, 128)
            acc = acc + jnp.sum(v * v, axis=0)
        return acc

    def turn(i, j):
        lags = pl.ds(pl.multiple_of(j * 128, 128), 128)
        for d in range(4):
            t = flat[max(i - 1, 0), pl.ds(pl.multiple_of(j * 512, 512) + d, 128, stride=4), :]
            t = t.astype(BF).T.reshape(4, 4, 8, 128)
            for c in range(2):
                xr[c, order[i], :, d, :, lags] = t[:, c]
            for c in range(2, 4):
                for q in range(4):
                    xr[c, q, order[i], d, :, lags] = t[q, c]

    def send_raw(i):
        if i == 0:
            pl.semaphore_wait(barrier, len(neighbours) + len(peers))
            for c in range(2):
                raw_block(c, x2).start()
        for c in range(2, 4):
            raw_piece(c, y2, order[i]).start()
            if i == 0:
                raw_second(c, 0).start()

    def tabulate(j, carry):
        lo = pltpu.roll(rows_ref[...], j * 16, 1)
        hi = pltpu.roll(rows_ref[...], j * 16 + 8, 1)
        both = jnp.concatenate([lo, hi], axis=0).astype(BF)
        for a in range(8):
            table[pl.ds(pl.multiple_of(a * 256 + j * 16, 16), 16), :] = both[:, 256 * (7 - a) : 256 * (7 - a) + WIDE]
        return carry

    lax.fori_loop(0, EARLY, tabulate, 0)

    squares = jnp.zeros((8, 128), F32)
    for q in range(4):
        first_loads[q].wait()
        squares = lax.fori_loop(4 * q, 4 * q + 4, lambda j, acc: widen(0, j, acc), squares)
    def turn_all(i):
        def step(j, carry):
            turn(i, j)
            return carry

        lax.fori_loop(0, 16, step, 0, unroll=2)
        send_raw(i)

    turn_all(0)
    for i in range(1, 4):
        loads[i].wait()
        if i < 3:
            loads[i + 1].start()
        squares = lax.fori_loop(0, 16, lambda j, acc, i=i: widen(i, j, acc), squares)

    en[0, 0] = squares
    en[0, 1] = masks[0] + masks[1] + masks[2] + masks[3]
    energy_copies = [
        remote(en.at[0], en.at[k], e_s.at[k], e_r.at[k], peers[k - 1]) for k in range(1, 8)
    ]
    for copy in energy_copies:
        copy.start()

    for i in range(1, 4):
        turn_all(i)

    lax.fori_loop(EARLY, 16, tabulate, 0)

    for copy in energy_copies:
        copy.wait_recv()
    total = jnp.sum(en[:, 0], axis=0)
    pairs_used = jnp.sum(en[:, 1], axis=0)
    energy = jnp.sum(total[:4] + total[4:], axis=1, keepdims=True)
    pairs_used = jnp.sum(pairs_used[:4], axis=1, keepdims=True)
    level = energy / (LAGS * jnp.maximum(pairs_used, 1.0)) + 0.1
    weight = lax.rsqrt(level)
    reach = weight * jnp.sqrt(energy)
    for d in range(4):
        ww[0, d] = jnp.broadcast_to(weight[d : d + 1], (8, 128))
        ww[1, d] = jnp.broadcast_to(0.25 * level[d : d + 1], (8, 128))
        ww[2, d] = jnp.broadcast_to(reach[d : d + 1], (8, 128))
    weight_copies = [remote(ww, wn.at[k], w_s.at[k], w_r.at[k], neighbours[k]) for k in range(4)]
    for copy in weight_copies:
        copy.start()
    for k in range(4):
        for c in range(4 if k else 2):
            raw_second(c, k).start()

    def scale_up(c):
        reach = jnp.maximum(jnp.max(ww[2], axis=0), jnp.max(wn[c, 2], axis=0))
        units = jnp.stack([reach, jnp.minimum(1.0, 2.0 * reach)]) * 2.0**-9.6
        units = jnp.maximum(units, 1e-30).astype(BF).astype(F32)
        unit[c, 0] = units
        unit[c, 1] = 1.0 / units

    def code(v, inverse_unit):
        t = v * inverse_unit
        t2 = t * t
        t4 = t2 * t2
        t = t4 * t4 * t2
        return jnp.where(v < 0.0, -t, t)

    def root(y, last, power):
        units = last[..., 127:128]
        size = jnp.exp((1.0 / power) * jnp.log(jnp.abs(y))) * units
        return jnp.where(y < 0.0, -size, size)

    def decode(ref):
        y = ref[...].astype(F32)
        return root(y, y[:, :, WIDE - 128 :], 10)

    def code_whole(v):
        largest = jnp.max(jnp.max(jnp.abs(v), axis=2, keepdims=True), axis=1, keepdims=True)
        u = (jnp.maximum(largest, 1e-30) * 2.0**-10.4).astype(BF).astype(F32)
        t = v * (1.0 / u)
        t2 = t * t
        t4 = t2 * t2
        t = t4 * t4 * t4
        lane = lax.broadcasted_iota(jnp.int32, (3, 8, WIDE), 2)
        return jnp.where(lane == WIDE - 1, u, jnp.where(v < 0.0, -t, t)).astype(BF)

    def decode_whole(ref):
        y = ref[...].astype(F32)
        return root(y, y[:, :, WIDE - 128 :], 12)

    def tile_sums(parts, slot, half, cols, sums):
        for at, raw, wq in parts:
            for d in range(4):
                hh = hil[slot, at + 8 * d : at + 8 * d + 8, half * 128 : half * 128 + 128]
                xx = raw[d, :, cols].astype(F32)
                inverse = lax.rsqrt(xx * xx + hh * hh + wq[1, d])
                sums = [sums[0] + wq[0, d] * xx, sums[1] + xx * inverse, sums[2] + hh * inverse]
        return sums

    def halves(n):
        for half in range(2):
            yield half, pl.ds(pl.multiple_of(n * 256 + half * 128, 128), 128)

    class FirstSums:
        def __init__(self, cs, far):
            self.cs, self.far = cs, far

        def before(self):
            if self.far:
                for c in self.cs:
                    weight_copies[c].wait_recv()
                    scale_up(c)
                    raw_block(c, x).wait_recv()

        def rows(self, c):
            return r1.at[c, 0] if self.far else xr.at[c, firsts[c][2]]

        def left(self):
            return [self.rows(c)[...].reshape(128, WIDE) for c in self.cs]

        def combine(self, n, slot):
            for i, c in enumerate(self.cs):
                wq = wn.at[c] if self.far else ww
                for half, cols in halves(n):
                    for b in range(4):
                        sums = [s1[c, b, k, :, cols] for k in range(3)] if self.far else [jnp.zeros((8, 128), F32)] * 3
                        sums = tile_sums([(i * 128 + b * 32, self.rows(c).at[b], wq)], slot, half, cols, sums)
                        for k in range(3):
                            if not self.far:
                                s1[c, b, k, :, cols] = sums[k]
                                continue
                            y = code(sums[k], unit[c, 1, min(k, 1)])
                            if isinstance(n, int) and n == 7 and half == 1:
                                lane = lax.broadcasted_iota(jnp.int32, (8, 128), 1)
                                y = jnp.where(lane == 127, unit[c, 0, min(k, 1)], y)
                            coded[c, b, k, :, cols] = y.astype(BF)

        def after(self):
            if self.far:
                for c in self.cs:
                    for k in range(2):
                        sums_first(c, k).start()

    class SecondSums:
        def __init__(self, k):
            self.k = k

        def before(self):
            for c in range(4):
                raw_second(c, self.k).wait_recv()
                if self.k == 3:
                    sums_first(c, self.k).wait_recv()

        def rows(self, c):
            b = second_order(c)[self.k]
            return xr.at[c, firsts[c][0], b], r1.at[c, 1, self.k]

        def left(self):
            return [r[...].reshape(32, WIDE) for c in range(4) for r in self.rows(c)]

        def combine(self, n, slot):
            for c in range(4):
                own, far = self.rows(c)
                for half, cols in halves(n):
                    parts = [(c * 64, own, ww), (c * 64 + 32, far, wn.at[c])]
                    if self.k == 3:
                        last = pl.ds(WIDE - 128, 128)
                        sums = [root(r2[c, self.k, k, :, cols].astype(F32), r2[c, self.k, k, :, last].astype(F32), 10) for k in range(3)]
                    else:
                        sums = [jnp.zeros((8, 128), F32)] * 3
                    sums = tile_sums(parts, slot, half, cols, sums)
                    for k in range(3):
                        s2[c, self.k, k, :, cols] = sums[k]

        def after(self):
            if self.k == 0:
                for k in range(2, 4):
                    for c in range(4):
                        sums_first(c, k).start()
            elif self.k == 1:
                for k in range(2):
                    for c in range(4):
                        stage_three(c, k)
            else:
                for c in range(4):
                    (stage_four, finish)[self.k - 2](c, self.k)

    def matmul(job, n, slot):
        cols = pl.ds(pl.multiple_of(n * 256, 256), 256)
        lhs = jnp.concatenate(job.left(), axis=0)
        hil[slot, : lhs.shape[0]] = jnp.dot(lhs, table[:, cols], preferred_element_type=F32)

    def sums_first(c, k):
        b = second_order(c)[k]
        return remote(coded.at[c, b], r2.at[c, k], b_s.at[c, k], b_r.at[c, k], at_first(c, firsts[c][2]))

    def sums_second(c, k):
        return remote(third.at[c, k], r3.at[c, k], c_s.at[c, k], c_r.at[c, k], at_second(c, seconds[c][1]))

    def sums_third(c):
        return remote(third.at[c, 2], r4.at[c], d_s.at[c], d_r.at[c], at_second(c, seconds[c][2]))

    def stage_three(c, k):
        sums_first(c, k).wait_recv()
        third[c, k] = code_whole(s2[c, k] + decode(r2.at[c, k]))
        sums_second(c, k).start()

    def stage_four(c, k):
        sums_first(c, 2).wait_recv()
        sums_second(c, 0).wait_recv()
        third[c, 2] = code_whole(s2[c, 2] + decode(r2.at[c, 2]) + decode_whole(r3.at[c, 0]))
        sums_third(c).start()

    def finish(c, k):
        sums_second(c, 1).wait_recv()
        sums_third(c).wait_recv()
        total = s2[c, 3] + decode_whole(r3.at[c, 1]) + decode_whole(r4.at[c])
        n = counts_column[8 * c : 8 * c + 8]
        sums_ref[0, pl.ds(8 * c, 8), :] = (total[0] / n)[:, :LAGS]
        sums_ref[1, pl.ds(8 * c, 8), :] = ((total[1] * total[1] + total[2] * total[2]) / (n * n))[:, :LAGS]

    counts = jnp.broadcast_to(jnp.maximum(counts_ref[...].astype(F32), 1.0), (32, 32))
    across = lax.broadcasted_iota(jnp.int32, (32, 32), 0) == lax.broadcasted_iota(jnp.int32, (32, 32), 1)
    counts_column = jnp.sum(jnp.where(across, counts, 0.0), axis=1, keepdims=True)

    jobs = [FirstSums((0, 1, 2, 3), False), FirstSums((0, 1), True), FirstSums((2, 3), True)]
    jobs += [SecondSums(k) for k in range(4)]
    matmul(jobs[0], 0, 0)
    for job, following in zip(jobs, jobs[1:] + [None]):

        def tiles(m, carry, job=job):
            matmul(job, 2 * m + 1, 1)
            job.combine(2 * m, 0)
            matmul(job, 2 * m + 2, 0)
            job.combine(2 * m + 1, 1)
            return carry

        lax.fori_loop(0, 3, tiles, 0)
        if following:
            following.before()
        matmul(job, 7, 1)
        job.combine(6, 0)
        if following:
            matmul(following, 0, 0)
        job.combine(7, 1)
        job.after()

    for copy in energy_copies + weight_copies:
        copy.wait_send()
    for c in range(4):
        raw_block(c, x).wait_send()
        for k in range(4):
            raw_second(c, k).wait_send()
            sums_first(c, k).wait_send()
        for k in range(2):
            sums_second(c, k).wait_send()
        sums_third(c).wait_send()


def shards(correlations, mask, counts):
    lag_major = jnp.transpose(correlations, (2, 0, 1))
    vmem = pl.BlockSpec(memory_space=pltpu.VMEM)
    dma = pltpu.SemaphoreType.DMA
    linear, coherence = pl.pallas_call(
        kernel,
        out_shape=pltpu.VMEM((2, 32, LAGS), F32),
        in_specs=[pl.BlockSpec(memory_space=pl.ANY), vmem, vmem],
        out_specs=vmem,
        scratch_shapes=[
            pltpu.VMEM((2, WIDE, 4, 128), BF),
            pltpu.VMEM((3, 8192, 128), F32),
            pltpu.VMEM((4, 4, 4, 4, 8, WIDE), BF),
            pltpu.VMEM((4, 2, 4, 4, 8, WIDE), BF),
            pltpu.VMEM((WIDE, WIDE), BF),
            pltpu.VMEM((4, 4, 3, 8, WIDE), F32),
            pltpu.VMEM((4, 4, 3, 8, WIDE), F32),
            pltpu.VMEM((4, 4, 3, 8, WIDE), BF),
            pltpu.VMEM((4, 4, 3, 8, WIDE), BF),
            pltpu.VMEM((4, 3, 3, 8, WIDE), BF),
            pltpu.VMEM((4, 2, 3, 8, WIDE), BF),
            pltpu.VMEM((4, 3, 8, WIDE), BF),
            pltpu.VMEM((8, 2, 8, 128), F32),
            pltpu.VMEM((3, 4, 8, 128), F32),
            pltpu.VMEM((4, 3, 4, 8, 128), F32),
            pltpu.VMEM((4, 2, 2, 8, 128), F32),
            pltpu.VMEM((2, 512, 256), F32),
            pltpu.VMEM((8, 4096), F32),
            dma((7,)),
            dma((4,)), dma((4,)),
            dma((4, 4)), dma((4, 4)),
            dma((4, 4)), dma((4, 4)),
            dma((4, 2)), dma((4, 2)),
            dma((4,)), dma((4,)),
            dma((8,)), dma((8,)),
            dma((4,)), dma((4,)),
        ],
        compiler_params=pltpu.CompilerParams(
            collective_id=0, has_side_effects=True, vmem_limit_bytes=58 * 2**20
        ),
    )(lag_major, mask, counts[None])
    return (linear * coherence, linear)


def solution(mesh):
    placed = (P("day", "pair", None), P("day", "pair"), P(("pair", "day")))
    return jax.shard_map(
        shards,
        mesh=mesh,
        in_specs=placed,
        out_specs=(P(("pair", "day"), None), P(("pair", "day"), None)),
        check_vma=False,
    )
```
